32 devices in a mesh: zero: 8 (over z, y), width: 4 (over x, core).
Axes of the slice: x: 2, y: 2, z: 4, core: 2. Of those that a mesh axis runs over, the one named last changes fastest.
Arguments:
- train_query: float32 [7168, 7168], P('zero', 'width'), may hold values from -0.09375 to 0.09375
- slow_query: float32 [7168, 7168], P('zero', 'width'), may hold values from -0.0625 to 0.0625
- train_key: float32 [7168, 1024], P('zero', 'width'), may hold values from -0.09375 to 0.09375
- slow_key: float32 [7168, 1024], P('zero', 'width'), may hold values from -0.0625 to 0.0625
- train_value: float32 [7168, 1024], P('zero', 'width'), may hold values from -0.09375 to 0.09375
- slow_value: float32 [7168, 1024], P('zero', 'width'), may hold values from -0.0625 to 0.0625
- norm_train: float32 [7168], P(('zero', 'width')), may hold values from 0.25 to 1.75
- norm_step: float32 [7168], P(('zero', 'width')), may hold values from -0.3 to 0.3
Outputs:
- ready_query: bfloat16 [7168, 7168], P(None, 'width')
- ready_key: bfloat16 [7168, 1024], P(None, 'width')
- ready_value: bfloat16 [7168, 1024], P(None, 'width')
- scale_query: float32 [7168], P('width')
- scale_key: float32 [1024], P('width')
- scale_value: float32 [1024], P('width')
- serve_norm: bfloat16 [7168], replicated
- latest_query: float32 [7168, 7168], P('zero', 'width')
- latest_key: float32 [7168, 1024], P('zero', 'width')
- latest_value: float32 [7168, 1024], P('zero', 'width')
The draws below stay inside these ranges and needn't reach their ends.
All inputs are finite; a program needn't handle non-finite values.
Results may differ from the reference program's by a relative error of at most 0.0004.
Values may be sent and summed in bfloat16 or wider, within the bound.
No kernel may reach another device: no remote copies, remote signals or barrier semaphores. Data moves between devices by JAX's collectives and lax.ppermute only.
A program may use at most 128 MiB of HBM per device.

```python
import jax
import jax.numpy as jnp
from jax import lax

D_MODEL = 7168
Q_DIM = 7168
KV_DIM = 1024


def strengthened(result, key, source, target, blocks, factor):
    def block_of(dim):
        return (jnp.arange(result.shape[dim]) // (result.shape[dim] // blocks)).reshape((-1,) + (1,) * (result.ndim - 1 - dim))

    near = jax.random.permutation(key, blocks)[block_of(target)]
    far = (block_of(target) + blocks // 2) % blocks
    return jnp.where((block_of(source) == near) | (block_of(source) == far), factor * result, result)


def levels(stream_key, extent, shards, smallest, high):
    def one(position, parts):
        heights = jax.random.uniform(jax.random.fold_in(jax.random.fold_in(stream_key, 6), position), (parts,), jnp.float32, smallest / len(shards), high / len(shards))
        return jnp.repeat(jnp.exp(heights), extent[position] // parts).reshape((-1,) + (1,) * (len(extent) - position - 1))

    factor_of = one(*shards[0])
    for cut in shards[1:]:
        factor_of = factor_of * one(*cut)
    return factor_of


def bell_draw(rng, extent, deviation, limit, shards=(), kind=jnp.bfloat16):
    entries = deviation * jax.random.normal(rng, extent, jnp.float32)
    if shards:
        entries = entries * levels(rng, extent, shards, -0.22, 0.18)
    return jnp.clip(entries, -limit, limit).astype(kind)


def noise_with(own_key, dims, deviation, bound, pieces, heavy, dtype=jnp.bfloat16):
    entries = deviation * jax.random.normal(own_key, dims, jnp.float32)
    if pieces:
        entries = entries * levels(own_key, dims, pieces, -0.22, 0.18)
    return jnp.clip(strengthened(entries, jax.random.fold_in(own_key, 3), *heavy), -bound, bound).astype(dtype)


def setup_inputs(seed: int = 0) -> dict:
    seeds = jax.random.split(jax.random.key(seed), 9)
    train_query = noise_with(seeds[0], (D_MODEL, Q_DIM), D_MODEL ** -0.5, 0.09375, ((0, 8), (1, 4)), (0, 1, 8, 2.0), jnp.float32)
    slow_query = bell_draw(seeds[1], (D_MODEL, Q_DIM), D_MODEL ** -0.5, 0.0625, ((0, 8), (1, 4)), jnp.float32)
    train_key = noise_with(seeds[2], (D_MODEL, KV_DIM), D_MODEL ** -0.5, 0.09375, ((0, 8), (1, 4)), (0, 1, 8, 2.0), jnp.float32)
    slow_key = bell_draw(seeds[3], (D_MODEL, KV_DIM), D_MODEL ** -0.5, 0.0625, ((0, 8), (1, 4)), jnp.float32)
    train_value = noise_with(seeds[4], (D_MODEL, KV_DIM), D_MODEL ** -0.5, 0.09375, ((0, 8), (1, 4)), (0, 1, 8, 2.0), jnp.float32)
    slow_value = bell_draw(seeds[5], (D_MODEL, KV_DIM), D_MODEL ** -0.5, 0.0625, ((0, 8), (1, 4)), jnp.float32)
    norm_train = jnp.clip(1.0 + 0.15 * jax.random.normal(seeds[6], (D_MODEL,), jnp.float32), 0.25, 1.75)
    norm_step = jnp.clip(jax.random.uniform(seeds[7], (D_MODEL,), jnp.float32, -0.3, 0.3) * levels(seeds[7], (D_MODEL,), ((0, 32),), -0.4, 0.0), -0.3, 0.3)
    return {"train_query": train_query, "slow_query": slow_query, "train_key": train_key, "slow_key": slow_key, "train_value": train_value, "slow_value": slow_value, "norm_train": norm_train, "norm_step": norm_step}


keep_rate = 0.5

def reference(train_query, slow_query, train_key, slow_key, train_value, slow_value, norm_train, norm_step):
    latest_query = keep_rate * slow_query + (1.0 - keep_rate) * train_query
    latest_key = keep_rate * slow_key + (1.0 - keep_rate) * train_key
    latest_value = keep_rate * slow_value + (1.0 - keep_rate) * train_value
    scale_query = jnp.sqrt(lax.optimization_barrier(jnp.sum(latest_query * latest_query, axis=0)))
    ready_query = (latest_query / scale_query).astype(jnp.bfloat16)
    scale_key = jnp.sqrt(lax.optimization_barrier(jnp.sum(latest_key * latest_key, axis=0)))
    ready_key = (latest_key / scale_key).astype(jnp.bfloat16)
    scale_value = jnp.sqrt(lax.optimization_barrier(jnp.sum(latest_value * latest_value, axis=0)))
    ready_value = (latest_value / scale_value).astype(jnp.bfloat16)
    serve_norm = (norm_train + norm_step).astype(jnp.bfloat16)
    return (ready_query, ready_key, ready_value, scale_query, scale_key, scale_value, serve_norm, latest_query, latest_key, latest_value)
```

```python
import functools

import jax
import jax.numpy as jnp
import numpy as np
from jax import lax
from jax.experimental import pallas as pl
from jax.experimental.pallas import tpu as pltpu
from jax.sharding import PartitionSpec as P

keep_rate = 0.5
LANES = 128


def ring_order(n, columns):
    rows = n // max(columns, 1)
    if columns < 2 or rows * columns != n or rows % 2:
        return list(range(n))
    order = [row * columns for row in range(rows)]
    for turn, row in enumerate(reversed(range(rows))):
        across = list(range(1, columns))
        order += [row * columns + c for c in (across if turn % 2 == 0 else across[::-1])]
    return order


def exchange(value, axis, n):
    return [value] + [
        lax.ppermute(value, axis, [(i, i ^ s) for i in range(n)]) for s in range(1, n)
    ]


def tree_sum(parts):
    while len(parts) > 1:
        parts = [a + b for a, b in zip(parts[::2], parts[1::2])]
    return parts[0]


def collect(parts, me):
    length = parts[0].shape[0]
    out = jnp.zeros((len(parts) * length,), parts[0].dtype)
    for s, part in enumerate(parts):
        out = lax.dynamic_update_slice(out, part, ((me ^ s) * length,))
    return out


def place_kernel(me_ref, block_ref, out_ref):
    out_ref[...] = block_ref[...]


def place_own(block, me, n):
    rows, cols = block.shape
    tile = rows
    for parts in (8, 7, 4, 2):
        if rows % (16 * parts) == 0:
            tile = rows // parts
            break
    steps = rows // tile
    return pl.pallas_call(
        place_kernel,
        out_shape=jax.ShapeDtypeStruct((n * rows, cols), block.dtype),
        grid_spec=pltpu.PrefetchScalarGridSpec(
            num_scalar_prefetch=1,
            grid=(steps,),
            in_specs=[pl.BlockSpec((tile, cols), lambda i, m: (i, 0))],
            out_specs=pl.BlockSpec((tile, cols), lambda i, m: (m[0] * steps + i, 0)),
        ),
        cost_estimate=pl.CostEstimate(
            flops=rows * cols * 16, bytes_accessed=4 * rows * cols, transcendentals=0
        ),
        name="place_own",
    )(me.reshape(1), block)


def body(
    order,
    widths,
    train_query, slow_query, train_key, slow_key, train_value, slow_value, norm_train, norm_step,
):
    n = len(order)
    me = lax.axis_index("zero")
    mine_w = lax.axis_index("width")

    latest_key = keep_rate * slow_key + (1.0 - keep_rate) * train_key
    latest_value = keep_rate * slow_value + (1.0 - keep_rate) * train_value
    latest_query = keep_rate * slow_query + (1.0 - keep_rate) * train_query

    kv_cols = latest_key.shape[1]
    kv_part = jnp.concatenate(
        [jnp.sum(latest_key * latest_key, axis=0), jnp.sum(latest_value * latest_value, axis=0)]
    )
    kv_scale = jnp.sqrt(tree_sum(exchange(kv_part, "zero", n)))
    scale_key, scale_value = kv_scale[:kv_cols], kv_scale[kv_cols:]

    q_part = jnp.sum(latest_query * latest_query, axis=0)
    norm = (norm_train + norm_step).astype(jnp.bfloat16).astype(jnp.float32)
    norm = collect(exchange(norm, "width", widths), mine_w)
    packed = exchange(jnp.concatenate([q_part, norm]), "zero", n)
    q_cols = q_part.shape[0]
    scale_query = jnp.sqrt(tree_sum([p[:q_cols] for p in packed]))
    serve_norm = collect([p[q_cols:].astype(jnp.bfloat16) for p in packed], me)

    narrow_key = (latest_key / scale_key).astype(jnp.bfloat16)
    narrow_value = (latest_value / scale_value).astype(jnp.bfloat16)
    narrow_query = (latest_query / scale_query).astype(jnp.bfloat16)

    outs = [place_own(x, me, n) for x in (narrow_query, narrow_key, narrow_value)]
    half = max(LANES, q_cols // 2 // LANES * LANES)
    chunks = [
        (1, 0, 1, narrow_key),
        (2, 0, -1, narrow_value),
        (0, 0, 1, narrow_query[:, :half]),
        (0, half, -1, narrow_query[:, half:]),
    ]
    forward = [(order[i], order[(i + 1) % n]) for i in range(n)]
    backward = [(b, a) for a, b in forward]
    position = np.argsort(np.array(order))
    here = jnp.asarray(position, jnp.int32)[me]
    at = jnp.asarray(order, jnp.int32)
    rows = narrow_query.shape[0]
    current = [c[3] for c in chunks]
    for step in range(1, n):
        source = {way: at[lax.rem(here + way * (n - step) + n, n)] if way > 0 else at[lax.rem(here + step, n)] for way in (1, -1)}
        for j, (which, col, way, _) in enumerate(chunks):
            current[j] = lax.ppermute(current[j], "zero", forward if way > 0 else backward)
            outs[which] = lax.dynamic_update_slice(
                outs[which], current[j], (source[way] * rows, col)
            )
    return (
        outs[0], outs[1], outs[2],
        scale_query, scale_key, scale_value, serve_norm,
        latest_query, latest_key, latest_value,
    )


def solution(mesh):
    n, widths = mesh.shape["zero"], mesh.shape["width"]
    two = P("zero", "width")
    flat = P(("zero", "width"))
    out_specs = (
        P(None, "width"), P(None, "width"), P(None, "width"),
        P("width"), P("width"), P("width"), P(),
        two, two, two,
    )
    order = ring_order(n, widths // 2)
    return jax.shard_map(
        functools.partial(body, order, widths),
        mesh=mesh,
        in_specs=(two,) * 6 + (flat,) * 2,
        out_specs=out_specs,
        check_vma=False,
    )
```
